32 devices in a mesh: rows: 2 (over x), cols: 8 (over z, y), frames: 2 (over core).
Axes of the slice: x: 2, y: 2, z: 4, core: 2. Of those that a mesh axis runs over, the one named last changes fastest.
Arguments:
- lidar_map: bfloat16 [8, 96, 192, 256], P('frames', ('rows', 'cols')), parts along dimension 0, may hold values from -6 to 6
- camera_map: bfloat16 [8, 96, 192, 80], P('frames', None, ('rows', 'cols')), parts along dimension 0, may hold values from -6 to 6
- joined_weight: bfloat16 [3, 3, 336, 256], replicated, may hold values from -0.15625 to 0.15625
- joined_bias: float32 [256], replicated, may hold values from -0.5 to 0.5
- block_weight: bfloat16 [3, 3, 256, 128], replicated, may hold values from -0.1875 to 0.1875
- block_bias: float32 [128], replicated, may hold values from -0.5 to 0.5
- down_weight: bfloat16 [3, 3, 128, 256], replicated, may hold values from -0.25 to 0.25
- down_bias: float32 [256], replicated, may hold values from -0.5 to 0.5
- proj_weight: bfloat16 [256, 128], replicated, may hold values from -0.5 to 0.5
- proj_bias: float32 [128], replicated, may hold values from -0.5 to 0.5
Outputs:
- encoded: bfloat16 [8, 96, 192, 256], P('frames', 'rows', 'cols'), parts along dimension 0
The draws below stay inside these ranges and needn't reach their ends.
There are 2 independent parts, one for each index of `frames`. The reference program is written for one: setup_inputs(seed, part) draws one part's arguments, and reference() takes and returns one part's arrays. A program takes and returns all parts, laid end to end along the dimension named above; an argument that names none is the same for every part. Nothing has to cross between parts.
All inputs are finite; a program needn't handle non-finite values.
Results may differ from the reference program's by a relative error of at most 0.0058.
Values may be sent and summed in bfloat16 or wider, within the bound.
A program may use at most 64 MiB of HBM per device.

```python
import jax
import jax.numpy as jnp
from jax import lax

FR = 4
LIDAR_CH = 256
CAM_CH = 80
JOINED_CH = 256
MID = 128
DEEP = 256
H = 96
W = 192


def levels(stream_key, dims, shards, least, high):
    def one(position, shards_of):
        steps = jax.random.uniform(jax.random.fold_in(jax.random.fold_in(stream_key, 6), position), (shards_of,), jnp.float32, least / len(shards), high / len(shards))
        return jnp.repeat(jnp.exp(steps), dims[position] // shards_of).reshape((-1,) + (1,) * (len(dims) - position - 1))

    gain = one(*shards[0])
    for cut in shards[1:]:
        gain = gain * one(*cut)
    return gain


def gaussian(rng, shape, spread, limit, shards=(), held_as=jnp.bfloat16):
    loudness = levels(rng, shape, shards, -0.22, 0.18) if shards else 1.0
    array = jax.random.normal(rng, shape, jnp.float32) * spread * loudness
    return jnp.minimum(jnp.maximum(array, -limit), limit).astype(held_as)


def setup_inputs(seed: int = 0, part: int = 0) -> dict:
    key_list = jax.random.split(jax.random.key(seed), 11)
    part_keys = jax.random.split(jax.random.fold_in(key_list[10], part), 11)
    lidar_map = gaussian(part_keys[0], (FR, H, W, LIDAR_CH), 1.0, 6.0, ((1, 16),))
    camera_map = gaussian(part_keys[1], (FR, H, W, CAM_CH), 1.0, 6.0, ((2, 16),))
    joined_weight = gaussian(key_list[2], (3, 3, LIDAR_CH + CAM_CH, JOINED_CH), (4 * (LIDAR_CH + CAM_CH)) ** -0.5, 0.15625)
    joined_bias = jnp.clip(jax.random.uniform(key_list[3], (JOINED_CH,), jnp.float32, -0.5, 0.5), -0.5, 0.5)
    block_weight = gaussian(key_list[4], (3, 3, JOINED_CH, MID), (4 * JOINED_CH) ** -0.5, 0.1875)
    block_bias = jnp.clip(jax.random.uniform(key_list[5], (MID,), jnp.float32, -0.5, 0.5), -0.5, 0.5)
    down_weight = gaussian(key_list[6], (3, 3, MID, DEEP), (4 * MID) ** -0.5, 0.25)
    down_bias = jnp.clip(jax.random.uniform(key_list[7], (DEEP,), jnp.float32, -0.5, 0.5), -0.5, 0.5)
    proj_weight = gaussian(key_list[8], (DEEP, MID), (DEEP // 2) ** -0.5, 0.5)
    proj_bias = jnp.clip(jax.random.uniform(key_list[9], (MID,), jnp.float32, -0.5, 0.5), -0.5, 0.5)
    return dict(lidar_map=lidar_map, camera_map=camera_map, joined_weight=joined_weight, joined_bias=joined_bias, block_weight=block_weight, block_bias=block_bias, down_weight=down_weight, down_bias=down_bias, proj_weight=proj_weight, proj_bias=proj_bias)


def conv_same(inputs, kernel, stride):
    return lax.conv_general_dilated(inputs, kernel, (stride, stride), ((1, 1), (1, 1)), dimension_numbers=("NHWC", "HWIO", "NHWC"), preferred_element_type=jnp.float32)


def reference(lidar_map, camera_map, joined_weight, joined_bias, block_weight, block_bias, down_weight, down_bias, proj_weight, proj_bias):
    stacked = jnp.concatenate([lidar_map, camera_map], axis=-1)
    joined = jax.nn.relu(conv_same(stacked, joined_weight, 1) + joined_bias).astype(jnp.bfloat16)
    block = jax.nn.relu(conv_same(joined, block_weight, 1) + block_bias).astype(jnp.bfloat16)
    deep = jax.nn.relu(conv_same(block, down_weight, 2) + down_bias).astype(jnp.bfloat16)
    branch = jax.nn.relu(jnp.einsum("fijc,cd->fijd", deep.astype(jnp.float32), proj_weight.astype(jnp.float32)) + proj_bias).astype(jnp.bfloat16)
    upsampled = jnp.repeat(jnp.repeat(branch, 2, axis=1), 2, axis=2)
    return jnp.concatenate([block, upsampled], axis=-1)
```

```python
import functools

import jax
import jax.numpy as jnp
from jax import lax
from jax.experimental import pallas as pl
from jax.experimental.pallas import tpu as pltpu
from jax.sharding import PartitionSpec as P

MESH = pl.DeviceIdType.MESH
ABOVE, BELOW = 3, 2


def exchange_kernel(
    R, C, lidar, cam, tile, cams,
    l_send, l_recv, l_own, c_send, c_recv, h_send, h_recv,
):
    frames, strip, _, _ = lidar.shape
    blocks = cams.shape[0]
    width = tile.shape[2]
    height = strip * C
    r, c = lax.axis_index("rows"), lax.axis_index("cols")
    me = r * C + c
    n = R * C

    barrier = pltpu.get_barrier_semaphore()

    @pl.loop(1, n)
    def _(k):
        other = lax.rem(me + k, n)
        pl.semaphore_signal(
            barrier, inc=1,
            device_id={"rows": other // C, "cols": lax.rem(other, C)},
            device_id_type=MESH,
        )

    pl.semaphore_wait(barrier, n - 1)

    def lidar_copy(f, k):
        to = lax.rem(c + k, C)
        return pltpu.make_async_remote_copy(
            src_ref=lidar.at[f, :, pl.ds(pl.multiple_of(to * width, 8), width), :],
            dst_ref=tile.at[f, pl.ds(ABOVE + c * strip, strip)],
            send_sem=l_send.at[f, k], recv_sem=l_recv.at[f, k],
            device_id={"cols": to}, device_id_type=MESH,
        )

    def lidar_arrival(f, k):
        by = lax.rem(c + C - k, C)
        ref = tile.at[f, pl.ds(ABOVE + by * strip, strip)]
        return pltpu.make_async_copy(ref, ref, l_recv.at[f, k])

    def own_copy(f):
        return pltpu.make_async_copy(
            lidar.at[f, :, pl.ds(pl.multiple_of(c * width, 8), width), :],
            tile.at[f, pl.ds(ABOVE + c * strip, strip)],
            l_own.at[f],
        )

    to_col, slot = me // blocks, lax.rem(me, blocks)

    def cam_refs(f, row):
        return (
            cam.at[f, pl.ds(row * height, height)],
            cams.at[slot, f, pl.ds(ABOVE, height)],
        )

    def cam_remote(f, row):
        src, dst = cam_refs(f, row)
        return pltpu.make_async_remote_copy(
            src_ref=src, dst_ref=dst,
            send_sem=c_send.at[f, row], recv_sem=c_recv.at[f, slot],
            device_id={"rows": row, "cols": to_col}, device_id_type=MESH,
        )

    def cam_local(f, row):
        src, dst = cam_refs(f, row)
        return pltpu.make_async_copy(src, dst, c_recv.at[f, slot])

    def cam_arrival(f, b):
        ref = cams.at[b, f, pl.ds(ABOVE, height)]
        return pltpu.make_async_copy(ref, ref, c_recv.at[f, b])

    def here(row):
        return jnp.logical_and(row == r, to_col == c)

    for f in range(frames):
        for row in range(R):
            @pl.when(jnp.logical_not(here(row)))
            def _():
                cam_remote(f, row).start()

            @pl.when(here(row))
            def _():
                cam_local(f, row).start()

        for k in range(1, C):
            lidar_copy(f, k).start()
        own_copy(f).start()

    @pl.when(r == 0)
    def _():
        tile[:, 0:ABOVE] = jnp.zeros((frames, ABOVE) + tile.shape[2:], tile.dtype)
        cams[:, :, 0:ABOVE] = jnp.zeros((blocks, frames, ABOVE) + cams.shape[3:], cams.dtype)

    @pl.when(r == R - 1)
    def _():
        tile[:, ABOVE + height:] = jnp.zeros((frames, BELOW) + tile.shape[2:], tile.dtype)
        cams[:, :, ABOVE + height:] = jnp.zeros(
            (blocks, frames, BELOW) + cams.shape[3:], cams.dtype
        )

    def rims(f, down):
        src, dst, size = (height, 0, ABOVE) if down else (ABOVE, ABOVE + height, BELOW)
        row = r + 1 if down else r - 1
        way = 0 if down else 1
        pairs = [(tile.at[f, pl.ds(src, size)], tile.at[f, pl.ds(dst, size)])]
        pairs += [
            (cams.at[b, f, pl.ds(src, size)], cams.at[b, f, pl.ds(dst, size)])
            for b in range(blocks)
        ]
        return [
            pltpu.make_async_remote_copy(
                src_ref=a, dst_ref=z,
                send_sem=h_send.at[f, way, i], recv_sem=h_recv.at[f, way, i],
                device_id={"rows": row}, device_id_type=MESH,
            )
            for i, (a, z) in enumerate(pairs)
        ]

    for f in range(frames):
        own_copy(f).wait()
        for k in range(1, C):
            lidar_arrival(f, k).wait()
        for b in range(blocks):
            cam_arrival(f, b).wait()

        @pl.when(r < R - 1)
        def _():
            for copy in rims(f, True):
                copy.start()

        @pl.when(r > 0)
        def _():
            for copy in rims(f, False):
                copy.start()

    for f in range(frames):
        @pl.when(r < R - 1)
        def _():
            for copy in rims(f, True):
                copy.wait_send()
            for copy in rims(f, False):
                copy.wait_recv()

        @pl.when(r > 0)
        def _():
            for copy in rims(f, False):
                copy.wait_send()
            for copy in rims(f, True):
                copy.wait_recv()

        for k in range(1, C):
            lidar_copy(f, k).wait_send()
        for row in range(R):
            @pl.when(jnp.logical_not(here(row)))
            def _():
                cam_remote(f, row).wait_send()


def exchange(lidar_map, camera_map):
    R, C = lax.axis_size("rows"), lax.axis_size("cols")
    frames, strip, grid_width, channels = lidar_map.shape
    _, _, cam_width, cam_channels = camera_map.shape
    height, width = strip * C, grid_width // C
    blocks = width // cam_width
    packed = cam_width * cam_channels
    lanes = max(d for d in range(1, 129) if packed % d == 0)
    cam = camera_map.reshape(frames, R * height, packed // lanes, lanes)
    rows = ABOVE + height + BELOW
    dma = pltpu.SemaphoreType.DMA
    tile, cams = pl.pallas_call(
        functools.partial(exchange_kernel, R, C),
        out_shape=(
            jax.ShapeDtypeStruct((frames, rows, width, channels), lidar_map.dtype),
            jax.ShapeDtypeStruct((blocks, frames, rows) + cam.shape[2:], cam.dtype),
        ),
        in_specs=[pl.BlockSpec(memory_space=pl.ANY)] * 2,
        out_specs=[pl.BlockSpec(memory_space=pltpu.VMEM)] * 2,
        scratch_shapes=[
            dma((frames, C)), dma((frames, C)), dma((frames,)),
            dma((frames, R)), dma((frames, blocks)),
            dma((frames, 2, 1 + blocks)), dma((frames, 2, 1 + blocks)),
        ],
        compiler_params=pltpu.CompilerParams(collective_id=0, has_side_effects=True),
    )(lidar_map, cam)
    cams = cams.reshape(blocks, frames, rows, cam_width, cam_channels)
    cams = cams.transpose(1, 2, 0, 3, 4).reshape(frames, rows, width, cam_channels)
    return jnp.concatenate([tile, cams], axis=-1)


def conv_valid(inputs, kernel, stride):
    return lax.conv_general_dilated(
        inputs,
        kernel,
        (stride, stride),
        "VALID",
        dimension_numbers=("NHWC", "HWIO", "NHWC"),
        preferred_element_type=jnp.float32,
    )


def inside(values, above, left, height, width):
    R, C = lax.axis_size("rows"), lax.axis_size("cols")
    row = lax.axis_index("rows") * height - above + jnp.arange(values.shape[1])
    col = lax.axis_index("cols") * width - left + jnp.arange(values.shape[2])
    rows_in = (row >= 0) & (row < R * height)
    cols_in = (col >= 0) & (col < C * width)
    return jnp.where((rows_in[:, None] & cols_in[None, :])[None, :, :, None], values, 0)


def local(
    lidar_map,
    camera_map,
    joined_weight,
    joined_bias,
    block_weight,
    block_bias,
    down_weight,
    down_bias,
    proj_weight,
    proj_bias,
):
    C = lax.axis_size("cols")
    height, width = lidar_map.shape[1] * C, lidar_map.shape[2] // C
    stacked = exchange(lidar_map, camera_map)
    right = [(i, i + 1) for i in range(C - 1)]
    left = [(i + 1, i) for i in range(C - 1)]
    padded = jnp.concatenate(
        [
            lax.ppermute(stacked[:, :, -ABOVE:], "cols", right),
            stacked,
            lax.ppermute(stacked[:, :, :BELOW], "cols", left),
        ],
        axis=2,
    )
    joined = jax.nn.relu(conv_valid(padded, joined_weight, 1) + joined_bias).astype(jnp.bfloat16)
    joined = inside(joined, 2, 2, height, width)
    block = jax.nn.relu(conv_valid(joined, block_weight, 1) + block_bias).astype(jnp.bfloat16)
    block = inside(block, 1, 1, height, width)
    deep = jax.nn.relu(conv_valid(block, down_weight, 2) + down_bias).astype(jnp.bfloat16)
    branch = jax.nn.relu(
        jnp.einsum("fijc,cd->fijd", deep, proj_weight, preferred_element_type=jnp.float32)
        + proj_bias
    ).astype(jnp.bfloat16)
    upsampled = jnp.repeat(jnp.repeat(branch, 2, axis=1), 2, axis=2)
    return jnp.concatenate([block[:, 1:, 1:], upsampled], axis=-1)


def solution(mesh):
    return jax.shard_map(
        local,
        mesh=mesh,
        in_specs=(
            P("frames", ("rows", "cols"), None, None),
            P("frames", None, ("rows", "cols"), None),
        ) + (P(),) * 8,
        out_specs=P("frames", "rows", "cols", None),
        check_vma=False,
    )
```

```python
import functools

import jax
import jax.numpy as jnp
from jax import lax
from jax.experimental import pallas as pl
from jax.experimental.pallas import tpu as pltpu
from jax.sharding import PartitionSpec as P

MESH = pl.DeviceIdType.MESH
ABOVE, BELOW = 3, 2


def exchange_kernel(
    R, C, lidar, cam, tile, cams,
    l_send, l_recv, l_own, c_send, c_recv, h_send, h_recv,
):
    frames, strip, _, _ = lidar.shape
    blocks = cams.shape[0]
    width = tile.shape[2]
    height = strip * C
    r, c = lax.axis_index("rows"), lax.axis_index("cols")
    me = r * C + c
    n = R * C

    barrier = pltpu.get_barrier_semaphore()

    @pl.loop(1, n)
    def _(k):
        other = lax.rem(me + k, n)
        pl.semaphore_signal(
            barrier, inc=1,
            device_id={"rows": other // C, "cols": lax.rem(other, C)},
            device_id_type=MESH,
        )

    pl.semaphore_wait(barrier, n - 1)

    def lidar_copy(f, k):
        to = lax.rem(c + k, C)
        return pltpu.make_async_remote_copy(
            src_ref=lidar.at[f, :, pl.ds(pl.multiple_of(to * width, 8), width), :],
            dst_ref=tile.at[f, pl.ds(ABOVE + c * strip, strip)],
            send_sem=l_send.at[f, k], recv_sem=l_recv.at[f, k],
            device_id={"cols": to}, device_id_type=MESH,
        )

    def lidar_arrival(f, k):
        by = lax.rem(c + C - k, C)
        ref = tile.at[f, pl.ds(ABOVE + by * strip, strip)]
        return pltpu.make_async_copy(ref, ref, l_recv.at[f, k])

    def own_copy(f):
        return pltpu.make_async_copy(
            lidar.at[f, :, pl.ds(pl.multiple_of(c * width, 8), width), :],
            tile.at[f, pl.ds(ABOVE + c * strip, strip)],
            l_own.at[f],
        )

    to_col, slot = me // blocks, lax.rem(me, blocks)

    def cam_refs(f, row):
        return (
            cam.at[f, pl.ds(row * height, height)],
            cams.at[slot, f, pl.ds(ABOVE, height)],
        )

    def cam_remote(f, row):
        src, dst = cam_refs(f, row)
        return pltpu.make_async_remote_copy(
            src_ref=src, dst_ref=dst,
            send_sem=c_send.at[f, row], recv_sem=c_recv.at[f, slot],
            device_id={"rows": row, "cols": to_col}, device_id_type=MESH,
        )

    def cam_local(f, row):
        src, dst = cam_refs(f, row)
        return pltpu.make_async_copy(src, dst, c_recv.at[f, slot])

    def cam_arrival(f, b):
        ref = cams.at[b, f, pl.ds(ABOVE, height)]
        return pltpu.make_async_copy(ref, ref, c_recv.at[f, b])

    def here(row):
        return jnp.logical_and(row == r, to_col == c)

    for f in range(frames):
        for row in range(R):
            @pl.when(jnp.logical_not(here(row)))
            def _():
                cam_remote(f, row).start()

            @pl.when(here(row))
            def _():
                cam_local(f, row).start()

        for k in range(1, C):
            lidar_copy(f, k).start()
        own_copy(f).start()

    @pl.when(r == 0)
    def _():
        tile[:, 0:ABOVE] = jnp.zeros((frames, ABOVE) + tile.shape[2:], tile.dtype)
        cams[:, :, 0:ABOVE] = jnp.zeros((blocks, frames, ABOVE) + cams.shape[3:], cams.dtype)

    @pl.when(r == R - 1)
    def _():
        tile[:, ABOVE + height:] = jnp.zeros((frames, BELOW) + tile.shape[2:], tile.dtype)
        cams[:, :, ABOVE + height:] = jnp.zeros(
            (blocks, frames, BELOW) + cams.shape[3:], cams.dtype
        )

    def rims(f, down):
        src, dst, size = (height, 0, ABOVE) if down else (ABOVE, ABOVE + height, BELOW)
        row = r + 1 if down else r - 1
        way = 0 if down else 1
        pairs = [(tile.at[f, pl.ds(src, size)], tile.at[f, pl.ds(dst, size)])]
        pairs += [
            (cams.at[b, f, pl.ds(src, size)], cams.at[b, f, pl.ds(dst, size)])
            for b in range(blocks)
        ]
        return [
            pltpu.make_async_remote_copy(
                src_ref=a, dst_ref=z,
                send_sem=h_send.at[f, way, i], recv_sem=h_recv.at[f, way, i],
                device_id={"rows": row}, device_id_type=MESH,
            )
            for i, (a, z) in enumerate(pairs)
        ]

    for f in range(frames):
        own_copy(f).wait()
        for k in range(1, C):
            lidar_arrival(f, k).wait()
        for b in range(blocks):
            cam_arrival(f, b).wait()

        @pl.when(r < R - 1)
        def _():
            for copy in rims(f, True):
                copy.start()

        @pl.when(r > 0)
        def _():
            for copy in rims(f, False):
                copy.start()

    for f in range(frames):
        @pl.when(r < R - 1)
        def _():
            for copy in rims(f, True):
                copy.wait_send()
            for copy in rims(f, False):
                copy.wait_recv()

        @pl.when(r > 0)
        def _():
            for copy in rims(f, False):
                copy.wait_send()
            for copy in rims(f, True):
                copy.wait_recv()

        for k in range(1, C):
            lidar_copy(f, k).wait_send()
        for row in range(R):
            @pl.when(jnp.logical_not(here(row)))
            def _():
                cam_remote(f, row).wait_send()


def exchange(lidar_map, camera_map):
    R, C = lax.axis_size("rows"), lax.axis_size("cols")
    frames, strip, grid_width, channels = lidar_map.shape
    _, _, cam_width, cam_channels = camera_map.shape
    height, width = strip * C, grid_width // C
    blocks = width // cam_width
    packed = cam_width * cam_channels
    lanes = max(d for d in range(1, 129) if packed % d == 0)
    cam = camera_map.reshape(frames, R * height, packed // lanes, lanes)
    rows = ABOVE + height + BELOW
    dma = pltpu.SemaphoreType.DMA
    tile, cams = pl.pallas_call(
        functools.partial(exchange_kernel, R, C),
        out_shape=(
            jax.ShapeDtypeStruct((frames, rows, width, channels), lidar_map.dtype),
            jax.ShapeDtypeStruct((blocks, frames, rows) + cam.shape[2:], cam.dtype),
        ),
        in_specs=[pl.BlockSpec(memory_space=pl.ANY)] * 2,
        out_specs=[pl.BlockSpec(memory_space=pltpu.VMEM)] * 2,
        scratch_shapes=[
            dma((frames, C)), dma((frames, C)), dma((frames,)),
            dma((frames, R)), dma((frames, blocks)),
            dma((frames, 2, 1 + blocks)), dma((frames, 2, 1 + blocks)),
        ],
        compiler_params=pltpu.CompilerParams(collective_id=0, has_side_effects=True),
    )(lidar_map, cam)
    cams = cams.reshape(blocks, frames, rows, cam_width, cam_channels)
    cams = cams.transpose(1, 2, 0, 3, 4).reshape(frames, rows, width, cam_channels)
    return tile, cams


EDGE = 8


def with_edges(cells):
    C = lax.axis_size("cols")
    right = [(i, i + 1) for i in range(C - 1)]
    left = [(i + 1, i) for i in range(C - 1)]
    before = jnp.swapaxes(cells[:, :, -ABOVE:], 1, 2)
    after = jnp.swapaxes(cells[:, :, :BELOW], 1, 2)
    before = lax.ppermute(before, "cols", right)
    after = lax.ppermute(after, "cols", left)
    before = jnp.pad(jnp.swapaxes(before, 1, 2), ((0, 0), (0, 1), (EDGE - ABOVE, 0), (0, 0)))
    after = jnp.pad(jnp.swapaxes(after, 1, 2), ((0, 0), (1, 0), (0, EDGE - BELOW), (0, 0)))
    edge = before + after
    cells = jnp.pad(cells, ((0, 0), (0, 1), (0, 0), (0, 0)))
    joint = jnp.concatenate([edge, cells], axis=2)
    return joint.reshape(joint.shape[0], joint.shape[1] * joint.shape[2], joint.shape[3])


def encode_kernel(
    R, C, span, height,
    lidar, cam, wj, bj, wb, bb, wd, bd, wp, bp, out, y, joined, block,
):
    width = span - EDGE
    lidar_channels = lidar.shape[2]
    r, c = lax.axis_index("rows"), lax.axis_index("cols")
    f32 = jnp.float32

    def dot(a, b):
        return jnp.dot(a, b, preferred_element_type=f32)

    def rows_at(start, count):
        return pl.ds(pl.multiple_of(start * span, span), count * span)

    def shifted(row, count, lanes):
        base = pl.multiple_of(row * span, 8)
        size = count * span
        before = pltpu.roll(y[0, pl.ds(base, size + 8), :lanes], 1, 0)[8:]
        after = pltpu.roll(y[2, pl.ds(base + 8, size + 8), :lanes], size + 7, 0)[:size]
        return before + y[1, pl.ds(base + 8, size), :lanes] + after

    def masked(values, row, first, wraps):
        shape = values.shape
        p = lax.broadcasted_iota(jnp.int32, shape, 0) + row * span
        i, j = p // span, p % span
        if wraps:
            over = j < EDGE - ABOVE
            i = jnp.where(over, i - 1, i)
            j = jnp.where(over, j + span, j)
        i = i + (r * height - first)
        j = j + (c * width - EDGE)
        ok = (i >= 0) & (i < R * height) & (j >= 0) & (j < C * width)
        return jnp.where(ok, values, 0.0)

    joined_rows, block_rows = height + 4, height + 1

    def steps(rows, limit):
        return max(d for d in range(1, limit + 1) if rows % d == 0)

    n1 = steps(joined_rows, 13)

    @pl.loop(0, joined_rows // n1)
    def _(t):
        row = t * n1
        for dj in range(3):
            total = None
            for di in range(3):
                at = rows_at(row + di, n1)
                term = dot(lidar[0, at, :], wj[di, dj, :lidar_channels, :])
                term += dot(cam[0, at, :], wj[di, dj, lidar_channels:, :])
                total = term if total is None else total + term
            y[dj, pl.ds(pl.multiple_of(row * span + 8, 8), n1 * span), :] = total

    @pl.loop(0, joined_rows // n1)
    def _(t):
        row = t * n1
        values = jnp.maximum(shifted(row, n1, y.shape[2]) + bj[...], 0.0)
        joined[rows_at(row, n1), :] = masked(values, row, 2, True).astype(joined.dtype)

    n2 = steps(block_rows + 1, 10)
    mid = wb.shape[3]

    @pl.loop(0, (block_rows + 1) // n2)
    def _(t):
        row = t * n2
        for dj in range(3):
            total = None
            for di in range(3):
                term = dot(joined[rows_at(row + di, n2), :], wb[di, dj])
                total = term if total is None else total + term
            y[dj, pl.ds(pl.multiple_of(row * span + 8, 8), n2 * span), :mid] = total

    m2 = steps(block_rows, 7)

    @pl.loop(0, block_rows // m2)
    def _(t):
        row = t * m2
        values = jnp.maximum(shifted(row, m2, mid) + bb[...], 0.0)
        values = masked(values, row, 1, False).astype(block.dtype)
        block[pl.ds(row, m2)] = values.reshape(m2, span, mid)

    half = height // 2
    n3 = steps(half, 8)
    deep_channels = wd.shape[3]

    @pl.loop(0, half // n3)
    def _(t):
        row = t * n3
        for dj in range(3):
            total = None
            for di in range(3):
                pairs = block[pl.ds(2 * row + (di // 2) * 2, 2 * n3)]
                pairs = pairs.reshape(n3, 2, span, mid)[:, di % 2]
                term = dot(pairs.reshape(n3 * span, mid), wd[di, dj])
                total = term if total is None else total + term
            y[dj, pl.ds(pl.multiple_of(row * span + 8, 8), n3 * span), :deep_channels] = total

    @pl.loop(0, half // n3)
    def _(t):
        row = t * n3
        deep = jnp.maximum(shifted(row, n3, deep_channels) + bd[...], 0.0).astype(block.dtype)
        branch = jnp.maximum(dot(deep, wp[...]) + bp[...], 0.0)
        odd = lax.broadcasted_iota(jnp.int32, branch.shape, 0) % 2 == 1
        branch = jnp.where(odd, pltpu.roll(branch, 1, 0), branch)
        branch = branch.reshape(n3, span, mid)[:, EDGE:].astype(out.dtype)
        branch = jnp.broadcast_to(branch[:, None], (n3, 2, width, mid))
        at = pl.ds(2 * row, 2 * n3)
        out[0, at, :, mid:] = branch.reshape(2 * n3, width, mid)
        kept = block[pl.ds(2 * row + 1, 2 * n3)].astype(f32)[:, EDGE:]
        out[0, at, :, :mid] = kept.astype(out.dtype)


def local(
    lidar_map,
    camera_map,
    joined_weight,
    joined_bias,
    block_weight,
    block_bias,
    down_weight,
    down_bias,
    proj_weight,
    proj_bias,
):
    R, C = lax.axis_size("rows"), lax.axis_size("cols")
    frames = lidar_map.shape[0]
    height, width = lidar_map.shape[1] * C, lidar_map.shape[2] // C
    span = width + EDGE
    tile, cams = exchange(lidar_map, camera_map)
    lidar, cam = with_edges(tile), with_edges(cams)
    wide = max(joined_weight.shape[3], down_weight.shape[3])
    mid = block_weight.shape[3]
    weights = [
        joined_weight, joined_bias[None], block_weight, block_bias[None],
        down_weight, down_bias[None], proj_weight, proj_bias[None],
    ]
    return pl.pallas_call(
        functools.partial(encode_kernel, R, C, span, height),
        grid=(frames,),
        out_shape=jax.ShapeDtypeStruct((frames, height, width, 2 * mid), lidar.dtype),
        in_specs=[
            pl.BlockSpec((1,) + lidar.shape[1:], lambda f: (f, 0, 0)),
            pl.BlockSpec((1,) + cam.shape[1:], lambda f: (f, 0, 0)),
        ] + [pl.BlockSpec(memory_space=pltpu.VMEM)] * 8,
        out_specs=pl.BlockSpec((1, height, width, 2 * mid), lambda f: (f, 0, 0, 0)),
        scratch_shapes=[
            pltpu.VMEM((3, (height + 4) * span + 16, wide), jnp.float32),
            pltpu.VMEM(((height + 4) * span, joined_weight.shape[3]), jnp.bfloat16),
            pltpu.VMEM((height + 2, span, mid), jnp.bfloat16),
        ],
        compiler_params=pltpu.CompilerParams(vmem_limit_bytes=48 << 20),
    )(lidar, cam, *weights)


def solution(mesh):
    return jax.shard_map(
        local,
        mesh=mesh,
        in_specs=(
            P("frames", ("rows", "cols"), None, None),
            P("frames", None, ("rows", "cols"), None),
        ) + (P(),) * 8,
        out_specs=P("frames", "rows", "cols", None),
        check_vma=False,
    )
```

```python
import functools

import jax
import jax.numpy as jnp
from jax import lax
from jax.experimental import pallas as pl
from jax.experimental.pallas import tpu as pltpu
from jax.sharding import PartitionSpec as P

MESH = pl.DeviceIdType.MESH
ABOVE, BELOW = 3, 2


def exchange_kernel(
    R, C, lidar, cam, tile, cams,
    l_send, l_recv, l_own, c_send, c_recv, h_send, h_recv,
):
    frames, strip, _, _ = lidar.shape
    blocks = cams.shape[0]
    width = tile.shape[2]
    height = strip * C
    r, c = lax.axis_index("rows"), lax.axis_index("cols")
    me = r * C + c
    n = R * C

    barrier = pltpu.get_barrier_semaphore()

    @pl.loop(1, n)
    def _(k):
        other = lax.rem(me + k, n)
        pl.semaphore_signal(
            barrier, inc=1,
            device_id={"rows": other // C, "cols": lax.rem(other, C)},
            device_id_type=MESH,
        )

    pl.semaphore_wait(barrier, n - 1)

    def lidar_copy(f, k):
        to = lax.rem(c + k, C)
        return pltpu.make_async_remote_copy(
            src_ref=lidar.at[f, :, pl.ds(pl.multiple_of(to * width, 8), width), :],
            dst_ref=tile.at[f, pl.ds(ABOVE + c * strip, strip)],
            send_sem=l_send.at[f, k], recv_sem=l_recv.at[f, k],
            device_id={"cols": to}, device_id_type=MESH,
        )

    def lidar_arrival(f, k):
        by = lax.rem(c + C - k, C)
        ref = tile.at[f, pl.ds(ABOVE + by * strip, strip)]
        return pltpu.make_async_copy(ref, ref, l_recv.at[f, k])

    def own_copy(f):
        return pltpu.make_async_copy(
            lidar.at[f, :, pl.ds(pl.multiple_of(c * width, 8), width), :],
            tile.at[f, pl.ds(ABOVE + c * strip, strip)],
            l_own.at[f],
        )

    to_col, slot = me // blocks, lax.rem(me, blocks)

    def cam_refs(f, row):
        return (
            cam.at[f, pl.ds(row * height, height)],
            cams.at[slot, f, pl.ds(ABOVE, height)],
        )

    def cam_remote(f, row):
        src, dst = cam_refs(f, row)
        return pltpu.make_async_remote_copy(
            src_ref=src, dst_ref=dst,
            send_sem=c_send.at[f, row], recv_sem=c_recv.at[f, slot],
            device_id={"rows": row, "cols": to_col}, device_id_type=MESH,
        )

    def cam_local(f, row):
        src, dst = cam_refs(f, row)
        return pltpu.make_async_copy(src, dst, c_recv.at[f, slot])

    def cam_arrival(f, b):
        ref = cams.at[b, f, pl.ds(ABOVE, height)]
        return pltpu.make_async_copy(ref, ref, c_recv.at[f, b])

    def here(row):
        return jnp.logical_and(row == r, to_col == c)

    for f in range(frames):
        for row in range(R):
            @pl.when(jnp.logical_not(here(row)))
            def _():
                cam_remote(f, row).start()

            @pl.when(here(row))
            def _():
                cam_local(f, row).start()

        for k in range(1, C):
            lidar_copy(f, k).start()
        own_copy(f).start()

    @pl.when(r == 0)
    def _():
        tile[:, 0:ABOVE] = jnp.zeros((frames, ABOVE) + tile.shape[2:], tile.dtype)
        cams[:, :, 0:ABOVE] = jnp.zeros((blocks, frames, ABOVE) + cams.shape[3:], cams.dtype)

    @pl.when(r == R - 1)
    def _():
        tile[:, ABOVE + height:] = jnp.zeros((frames, BELOW) + tile.shape[2:], tile.dtype)
        cams[:, :, ABOVE + height:] = jnp.zeros(
            (blocks, frames, BELOW) + cams.shape[3:], cams.dtype
        )

    def rims(f, down):
        src, dst, size = (height, 0, ABOVE) if down else (ABOVE, ABOVE + height, BELOW)
        row = r + 1 if down else r - 1
        way = 0 if down else 1
        pairs = [(tile.at[f, pl.ds(src, size)], tile.at[f, pl.ds(dst, size)])]
        pairs += [
            (cams.at[b, f, pl.ds(src, size)], cams.at[b, f, pl.ds(dst, size)])
            for b in range(blocks)
        ]
        return [
            pltpu.make_async_remote_copy(
                src_ref=a, dst_ref=z,
                send_sem=h_send.at[f, way, i], recv_sem=h_recv.at[f, way, i],
                device_id={"rows": row}, device_id_type=MESH,
            )
            for i, (a, z) in enumerate(pairs)
        ]

    for f in range(frames):
        own_copy(f).wait()
        for k in range(1, C):
            lidar_arrival(f, k).wait()
        for b in range(blocks):
            cam_arrival(f, b).wait()

        @pl.when(r < R - 1)
        def _():
            for copy in rims(f, True):
                copy.start()

        @pl.when(r > 0)
        def _():
            for copy in rims(f, False):
                copy.start()

    for f in range(frames):
        @pl.when(r < R - 1)
        def _():
            for copy in rims(f, True):
                copy.wait_send()
            for copy in rims(f, False):
                copy.wait_recv()

        @pl.when(r > 0)
        def _():
            for copy in rims(f, False):
                copy.wait_send()
            for copy in rims(f, True):
                copy.wait_recv()

        for k in range(1, C):
            lidar_copy(f, k).wait_send()
        for row in range(R):
            @pl.when(jnp.logical_not(here(row)))
            def _():
                cam_remote(f, row).wait_send()


def exchange(lidar_map, camera_map):
    R, C = lax.axis_size("rows"), lax.axis_size("cols")
    frames, strip, grid_width, channels = lidar_map.shape
    _, _, cam_width, cam_channels = camera_map.shape
    height, width = strip * C, grid_width // C
    blocks = width // cam_width
    packed = cam_width * cam_channels
    lanes = max(d for d in range(1, 129) if packed % d == 0)
    cam = camera_map.reshape(frames, R * height, packed // lanes, lanes)
    rows = ABOVE + height + BELOW
    dma = pltpu.SemaphoreType.DMA
    tile, cams = pl.pallas_call(
        functools.partial(exchange_kernel, R, C),
        out_shape=(
            jax.ShapeDtypeStruct((frames, rows, width, channels), lidar_map.dtype),
            jax.ShapeDtypeStruct((blocks, frames, rows) + cam.shape[2:], cam.dtype),
        ),
        in_specs=[pl.BlockSpec(memory_space=pl.ANY)] * 2,
        out_specs=[pl.BlockSpec(memory_space=pltpu.VMEM)] * 2,
        scratch_shapes=[
            dma((frames, C)), dma((frames, C)), dma((frames,)),
            dma((frames, R)), dma((frames, blocks)),
            dma((frames, 2, 1 + blocks)), dma((frames, 2, 1 + blocks)),
        ],
        compiler_params=pltpu.CompilerParams(collective_id=0, has_side_effects=True),
    )(lidar_map, cam)
    cams = cams.reshape(blocks, frames, rows, cam_width, cam_channels)
    cams = cams.transpose(1, 2, 0, 3, 4).reshape(frames, rows, width, cam_channels)
    return tile, cams


EDGE = 8


def with_edges(cells):
    C = lax.axis_size("cols")
    right = [(i, i + 1) for i in range(C - 1)]
    left = [(i + 1, i) for i in range(C - 1)]
    before = jnp.swapaxes(cells[:, :, -ABOVE:], 1, 2)
    after = jnp.swapaxes(cells[:, :, :BELOW], 1, 2)
    before = lax.ppermute(before, "cols", right)
    after = lax.ppermute(after, "cols", left)
    before = jnp.pad(jnp.swapaxes(before, 1, 2), ((0, 0), (0, 1), (EDGE - ABOVE, 0), (0, 0)))
    after = jnp.pad(jnp.swapaxes(after, 1, 2), ((0, 0), (1, 0), (0, EDGE - BELOW), (0, 0)))
    edge = before + after
    cells = jnp.pad(cells, ((0, 0), (0, 1), (0, 0), (0, 0)))
    joint = jnp.concatenate([edge, cells], axis=2)
    return joint.reshape(joint.shape[0], joint.shape[1] * joint.shape[2], joint.shape[3])


def encode_kernel(
    R, C, span, height,
    lidar, cam, wj, bj, wb, bb, wd, bd, wp, bp, out, y, joined, block,
):
    width = span - EDGE
    lidar_channels = lidar.shape[2]
    r, c = lax.axis_index("rows"), lax.axis_index("cols")
    f32 = jnp.float32

    def dot(a, b):
        return jnp.dot(a, b, preferred_element_type=f32)

    def rows_at(start, count):
        return pl.ds(pl.multiple_of(start * span, span), count * span)

    def shifted(row, count, lanes):
        base = pl.multiple_of(row * span, 8)
        size = count * span
        before = pltpu.roll(y[0, pl.ds(base, size + 8), :lanes], 1, 0)[8:]
        after = pltpu.roll(y[2, pl.ds(base + 8, size + 8), :lanes], size + 7, 0)[:size]
        return before + y[1, pl.ds(base + 8, size), :lanes] + after

    def masked(values, row, first, wraps):
        flat = values.shape
        values = values.reshape(flat[0] // span, span, flat[1])
        i = lax.broadcasted_iota(jnp.int32, values.shape, 0)
        j = lax.broadcasted_iota(jnp.int32, (1, span, flat[1]), 1)
        high = R * height - (row + r * height - first)
        low = high - R * height
        if wraps:
            over = j < EDGE - ABOVE
            i = i - jnp.where(over, 1, 0)
            j = jnp.where(over, j + span, j)
        j = j + (c * width - EDGE)
        ok = (i >= low) & (i < high) & ((j >= 0) & (j < C * width))
        return jnp.where(ok, values, 0.0).reshape(flat)

    joined_rows, block_rows = height + 4, height + 1

    def steps(rows, limit):
        return max(d for d in range(1, limit + 1) if rows % d == 0)

    n1 = steps(joined_rows, 13)

    @pl.loop(0, joined_rows // n1)
    def _(t):
        row = t * n1
        for dj in range(3):
            total = None
            for di in range(3):
                at = rows_at(row + di, n1)
                term = dot(lidar[0, at, :], wj[di, dj, :lidar_channels, :])
                term += dot(cam[0, at, :], wj[di, dj, lidar_channels:, :])
                total = term if total is None else total + term
            y[dj, pl.ds(pl.multiple_of(row * span + 8, 8), n1 * span), :] = total

    @pl.loop(0, joined_rows // n1)
    def _(t):
        row = t * n1
        values = jnp.maximum(shifted(row, n1, y.shape[2]) + bj[...], 0.0)
        joined[rows_at(row, n1), :] = masked(values, row, 2, True).astype(joined.dtype)

    n2 = steps(block_rows + 1, 10)
    mid = wb.shape[3]

    @pl.loop(0, (block_rows + 1) // n2)
    def _(t):
        row = t * n2
        for dj in range(3):
            total = None
            for di in range(3):
                term = dot(joined[rows_at(row + di, n2), :], wb[di, dj])
                total = term if total is None else total + term
            y[dj, pl.ds(pl.multiple_of(row * span + 8, 8), n2 * span), :mid] = total

    m2 = steps(block_rows, 7)

    @pl.loop(0, block_rows // m2)
    def _(t):
        row = t * m2
        values = jnp.maximum(shifted(row, m2, mid) + bb[...], 0.0)
        values = masked(values, row, 1, False).astype(block.dtype)
        block[pl.ds(row, m2)] = values.reshape(m2, span, mid)

    half = height // 2
    n3 = steps(half, 8)
    deep_channels = wd.shape[3]

    @pl.loop(0, half // n3)
    def _(t):
        row = t * n3
        for dj in range(3):
            total = None
            for di in range(3):
                pairs = block[pl.ds(2 * row + (di // 2) * 2, 2 * n3)]
                pairs = pairs.reshape(n3, 2, span, mid)[:, di % 2]
                term = dot(pairs.reshape(n3 * span, mid), wd[di, dj])
                total = term if total is None else total + term
            y[dj, pl.ds(pl.multiple_of(row * span + 8, 8), n3 * span), :deep_channels] = total

    @pl.loop(0, half // n3)
    def _(t):
        row = t * n3
        deep = jnp.maximum(shifted(row, n3, deep_channels) + bd[...], 0.0).astype(block.dtype)
        branch = jnp.maximum(dot(deep, wp[...]) + bp[...], 0.0)
        odd = lax.broadcasted_iota(jnp.int32, branch.shape, 0) % 2 == 1
        branch = jnp.where(odd, pltpu.roll(branch, 1, 0), branch)
        branch = branch.reshape(n3, span, mid)[:, EDGE:].astype(out.dtype)
        branch = jnp.broadcast_to(branch[:, None], (n3, 2, width, mid))
        at = pl.ds(2 * row, 2 * n3)
        out[0, at, :, mid:] = branch.reshape(2 * n3, width, mid)
        kept = block[pl.ds(2 * row + 1, 2 * n3)].astype(f32)[:, EDGE:]
        out[0, at, :, :mid] = kept.astype(out.dtype)


def local(
    lidar_map,
    camera_map,
    joined_weight,
    joined_bias,
    block_weight,
    block_bias,
    down_weight,
    down_bias,
    proj_weight,
    proj_bias,
):
    R, C = lax.axis_size("rows"), lax.axis_size("cols")
    frames = lidar_map.shape[0]
    height, width = lidar_map.shape[1] * C, lidar_map.shape[2] // C
    span = width + EDGE
    tile, cams = exchange(lidar_map, camera_map)
    lidar, cam = with_edges(tile), with_edges(cams)
    wide = max(joined_weight.shape[3], down_weight.shape[3])
    mid = block_weight.shape[3]
    weights = [
        joined_weight, joined_bias[None], block_weight, block_bias[None],
        down_weight, down_bias[None], proj_weight, proj_bias[None],
    ]
    return pl.pallas_call(
        functools.partial(encode_kernel, R, C, span, height),
        grid=(frames,),
        out_shape=jax.ShapeDtypeStruct((frames, height, width, 2 * mid), lidar.dtype),
        in_specs=[
            pl.BlockSpec((1,) + lidar.shape[1:], lambda f: (f, 0, 0)),
            pl.BlockSpec((1,) + cam.shape[1:], lambda f: (f, 0, 0)),
        ] + [pl.BlockSpec(memory_space=pltpu.VMEM)] * 8,
        out_specs=pl.BlockSpec((1, height, width, 2 * mid), lambda f: (f, 0, 0, 0)),
        scratch_shapes=[
            pltpu.VMEM((3, (height + 4) * span + 16, wide), jnp.float32),
            pltpu.VMEM(((height + 4) * span, joined_weight.shape[3]), jnp.bfloat16),
            pltpu.VMEM((height + 2, span, mid), jnp.bfloat16),
        ],
        compiler_params=pltpu.CompilerParams(vmem_limit_bytes=48 << 20),
    )(lidar, cam, *weights)


def solution(mesh):
    return jax.shard_map(
        local,
        mesh=mesh,
        in_specs=(
            P("frames", ("rows", "cols"), None, None),
            P("frames", None, ("rows", "cols"), None),
        ) + (P(),) * 8,
        out_specs=P("frames", "rows", "cols", None),
        check_vma=False,
    )
```
